32 devices in a mesh: tok: 4 (over y, x), row: 2 (over core), col: 4 (over z).
Axes of the slice: x: 2, y: 2, z: 4, core: 2. Of those that a mesh axis runs over, the one named last changes fastest.
Arguments:
- activations: bfloat16 [2048, 4096], P(('tok', 'col'), 'row'), may hold values from -6 to 6
- grads_t: bfloat16 [4, 7392, 2048], P(None, 'col', ('tok', 'row')), may hold values from -0.14941406 to 0.14941406
Outputs:
- weight_grad: float32 [4, 7392, 4096], P('tok', 'col', 'row')
The draws below stay inside these ranges and needn't reach their ends.
All inputs are finite; a program needn't handle non-finite values.
Results may differ from the reference program's by a relative error of at most 0.0003.
Values may be sent and summed in bfloat16 or wider, within the bound.
A program may use at most 128 MiB of HBM per device.

```python
import jax
import jax.numpy as jnp

D = 4096
FF = 29568
TOK_DEV = 512
TOKENS = 2048
N_TOK = 4


def raised(drawn, stream_key, source, target, shards_of, factor):
    def block_of(dim):
        return (jnp.arange(drawn.shape[dim]) // (drawn.shape[dim] // shards_of)).reshape((-1,) + (1,) * (drawn.ndim - 1 - dim))

    first = jax.random.permutation(stream_key, shards_of)[block_of(target)]
    second = (block_of(target) + shards_of // 2) % shards_of
    return jnp.where((block_of(source) == first) | (block_of(source) == second), factor * drawn, drawn)


def shard_levels(stream_key, extent, split, low, high):
    def one(dim, shards_of):
        draws = jax.random.uniform(jax.random.fold_in(jax.random.fold_in(stream_key, 6), dim), (shards_of,), jnp.float32, low / len(split), high / len(split))
        return jnp.repeat(jnp.exp(draws), extent[dim] // shards_of).reshape((-1,) + (1,) * (len(extent) - dim - 1))

    level = one(*split[0])
    for cut in split[1:]:
        level = level * one(*cut)
    return level


def noise(rng, dims, spread, bound, split=(), kind=jnp.bfloat16):
    factor_of = shard_levels(rng, dims, split, -0.22, 0.18) if split else 1.0
    entries = jax.random.normal(rng, dims, jnp.float32) * spread * factor_of
    return jnp.minimum(jnp.maximum(entries, -bound), bound).astype(kind)


def gaussian_with(rng, dims, spread, reach, shards, heavy, held_as=jnp.bfloat16):
    values = spread * jax.random.normal(rng, dims, jnp.float32)
    if shards:
        values = values * shard_levels(rng, dims, shards, -0.22, 0.18)
    return jnp.clip(raised(values, jax.random.fold_in(rng, 3), *heavy), -reach, reach).astype(held_as)


def setup_inputs(seed: int = 0) -> dict:
    splits = jax.random.split(jax.random.key(seed), 3)
    return {
        "activations": noise(splits[0], (TOKENS, D), 1.0, 6.0, ((0, 16), (1, 2))),
        "grads_t": gaussian_with(splits[1], (N_TOK, FF // N_TOK, TOKENS), 0.025, 0.14941406, ((1, 4), (2, 8)), (2, 0, 4, 2.0)),
    }


def reference(activations, grads_t):
    flat = grads_t.reshape(FF, TOKENS)
    total = jnp.zeros((FF, D), jnp.float32)
    for group in range(N_TOK):
        block = flat[:, group * TOK_DEV:(group + 1) * TOK_DEV]
        rows = activations[group * TOK_DEV:(group + 1) * TOK_DEV]
        total = total + jnp.dot(block, rows, preferred_element_type=jnp.float32)
    return total.reshape(N_TOK, FF // N_TOK, D)
```

```python
import jax
import jax.numpy as jnp
from jax import lax
from jax.sharding import PartitionSpec as P


def body(activations, grads_t):
    groups, units, own = grads_t.shape
    mine = lax.all_to_all(grads_t, "tok", split_axis=0, concat_axis=0, tiled=True)
    mine = lax.all_gather(mine, "row", axis=1, tiled=False)
    acts_all = lax.all_gather(activations, "col", axis=0, tiled=True)
    acts_all = lax.all_gather(acts_all, "tok", axis=0, tiled=True)
    flat = mine.transpose(2, 0, 1, 3).reshape(units, mine.size // units)
    tile = jnp.dot(flat, acts_all, preferred_element_type=jnp.float32)
    return tile[None]


def solution(mesh):
    return jax.shard_map(
        body,
        mesh=mesh,
        in_specs=(P(("tok", "col"), "row"), P(None, "col", ("tok", "row"))),
        out_specs=P("tok", "col", "row"),
        check_vma=False,
    )
```

```python
import functools

import jax
import jax.numpy as jnp
from jax import lax
from jax.experimental import pallas as pl
from jax.experimental.pallas import tpu as pltpu
from jax.sharding import PartitionSpec as P

MESH = pl.DeviceIdType.MESH


def ring_map(place, n):
    if n % 4:
        return place
    return place + ((place % 4) // 2) * (1 - 2 * (place % 2))


def kernel(n, m, acts, grads, out, first, last, held, total,
           local_sem, zsend, zrecv, rsend, rrecv, gsend, grecv, psend, out_sem):
    k, r, c = lax.axis_index("tok"), lax.axis_index("row"), lax.axis_index("col")
    place = ring_map(k, n)
    rows, wide = acts.shape
    quarter = wide // 4
    chunk = grads.shape[2]
    up, down = c + 1 < m, c > 0
    reach = ((n // 2, n - 1 - n // 2), (n - 1 - n // 2, n // 2))
    hops = n // 2

    def member(offset):
        return ring_map((place + offset + 2 * n) % n, n)

    barrier = pltpu.get_barrier_semaphore()
    for j in range(1, n):
        pl.semaphore_signal(barrier, inc=1, device_id={"tok": (k + j) % n}, device_id_type=MESH)
    pl.semaphore_signal(barrier, inc=1, device_id={"row": 1 - r}, device_id_type=MESH)

    @pl.when(up)
    def _():
        pl.semaphore_signal(barrier, inc=1, device_id={"col": c + 1}, device_id_type=MESH)

    @pl.when(down)
    def _():
        pl.semaphore_signal(barrier, inc=1, device_id={"col": c - 1}, device_id_type=MESH)

    def span(tok, col):
        return pl.ds(pl.multiple_of((tok * m + col) * rows, rows), rows)

    own = span(k, c)
    loads = []
    for q in range(4):
        dst = (first, last)[q // 2].at[q % 2, own, :]
        loads.append(pltpu.make_async_copy(acts.at[:, pl.ds(q * quarter, quarter)], dst, local_sem.at[q]))
    mine = pltpu.make_async_copy(grads.at[k], held.at[k, r], local_sem.at[4])
    for load in loads[2:] + loads[:2] + [mine]:
        load.start()
    for load in loads:
        load.wait()

    @pl.when(up & down)
    def _():
        pl.semaphore_wait(barrier, n + 2)

    @pl.when(jnp.logical_not(up & down))
    def _():
        pl.semaphore_wait(barrier, n + 1)

    def z_copy(item, tok, col, way):
        buf = first if isinstance(item, int) and item == 0 else last
        where = buf.at[:, span(tok, col), :]
        return pltpu.make_async_remote_copy(
            where, where, zsend.at[way, item, col], zrecv.at[item, col],
            device_id={"col": c + 1 - 2 * way}, device_id_type=MESH)

    def z_start(item, tok):
        @pl.when(up)
        def _():
            z_copy(item, tok, c, 0).start()

        @pl.when(down)
        def _():
            z_copy(item, tok, c, 1).start()

    def z_round(s, item, tok):
        below, above = c - 1 - s, c + 1 + s

        @pl.when(below >= 0)
        def _():
            z_copy(item, tok, below, 0).wait_recv()

            @pl.when(up)
            def _():
                z_copy(item, tok, below, 0).start()

        @pl.when(above < m)
        def _():
            z_copy(item, tok, above, 1).wait_recv()

            @pl.when(down)
            def _():
                z_copy(item, tok, above, 1).start()

    def ring_copy(line, col, offset, half, way):
        buf = last if isinstance(line, int) and line == m else first
        tok = member(offset)
        where = buf.at[half, span(tok, col), :]
        return pltpu.make_async_remote_copy(
            where, where, rsend.at[way, line, tok, half], rrecv.at[line, tok, half],
            device_id={"tok": member(1 - 2 * way)}, device_id_type=MESH)

    def ring_start(line, col):
        for half in range(2):
            for way in range(2):
                which = half if way == 0 else 1 - half
                if reach[which][way] >= 1:
                    ring_copy(line, col, 0, which, way).start()

    def ring_step(line, col, t):
        for half in range(2):
            for way in range(2):
                which = half if way == 0 else 1 - half
                if reach[which][way] >= t:
                    offset = -t if way == 0 else t
                    ring_copy(line, col, offset, which, way).wait_recv()
                    if reach[which][way] > t:
                        ring_copy(line, col, offset, which, way).start()

    def ring_sent(line, col):
        for half in range(2):
            for way in range(2):
                for t in range(reach[half][way]):
                    ring_copy(line, col, -t if way == 0 else t, half, way).wait_send()

    def at_distance(d, do):
        @pl.when(c - d >= 0)
        def _():
            do(c - d, c - d)

        @pl.when((c + d < m) & (d > 0))
        def _():
            do(c + d, c + d)

    def g_send(j):
        to = (k + j) % n
        return pltpu.make_async_remote_copy(
            grads.at[to], held.at[k, r], gsend.at[j], grecv.at[k, r],
            device_id={"tok": to}, device_id_type=MESH)

    def g_recv(tok):
        where = held.at[tok, r]
        return pltpu.make_async_remote_copy(
            where, where, gsend.at[0], grecv.at[tok, r],
            device_id={"row": 1 - r}, device_id_type=MESH)

    def partner(tok, side):
        where = held.at[tok, side]
        return pltpu.make_async_remote_copy(
            where, where, psend.at[tok], grecv.at[tok, side],
            device_id={"row": 1 - r}, device_id_type=MESH)

    ring_start(m, c)
    z_start(0, k)
    z_start(1, k)
    ring_start(c, c)
    mine.wait()
    partner(k, r).start()
    for t in range(1, hops + 1):
        ring_step(m, c, t)
        if t == 1:
            for j in sorted(range(1, n), key=lambda j: (min(j, n - j), j)):
                g_send(j).start()
        z_start(1 + (n - t), member(-t))
        if 2 * t != n:
            z_start(1 + t, member(t))
        if t == 1:
            total[...] = jnp.zeros_like(total)

    def item_order():
        order = [0]
        for t in range(1, hops + 1):
            order.append(n - t)
            if 2 * t != n:
                order.append(t)
        return order

    def whole_round(s):
        z_round(s, 0, k)
        at_distance(s + 1, ring_start)
        for j in item_order():
            z_round(s, 1 + j, member(j))

    def compute(buf, base, tok, side):
        at = pl.ds(pl.multiple_of((tok * 2 + side) * chunk, chunk), chunk)
        step = min(256, quarter)
        for half in range(2):
            @pl.loop(0, quarter // step)
            def _(i):
                cols = pl.ds(pl.multiple_of(i * step, step), step)
                outc = pl.ds(pl.multiple_of((base + half) * quarter + i * step, step), step)
                total[:, outc] += jnp.dot(
                    held[tok, side], buf[half, at, cols], preferred_element_type=jnp.float32)

    @pl.loop(0, m - 2)
    def _(s):
        whole_round(s)

    for j in sorted(range(1, n), key=lambda j: (min(j, n - j), j)):
        tok = (k + n - j) % n
        g_recv(tok).wait_recv()
        partner(tok, r).start()

    near = (2 * c) // m

    @pl.loop(0, m - 1)
    def _(d):
        at_distance(d, functools.partial(ring_step, t=1))

    @pl.loop(0, n)
    def _(j):
        partner((k + j) % n, 1 - r).wait_recv()

    @pl.loop(0, n)
    def _(j):
        compute(last, 2, j, near)

    z_round(m - 2, 0, k)
    at_distance(m - 1, ring_start)
    at_distance(m - 1, functools.partial(ring_step, t=1))
    for j in item_order():
        z_round(m - 2, 1 + j, member(j))
    for t in range(2, hops + 1):
        @pl.loop(0, m)
        def _(d):
            at_distance(d, functools.partial(ring_step, t=t))

    @pl.loop(0, n)
    def _(j):
        compute(last, 2, j, 1 - near)

    @pl.loop(0, 2 * n)
    def _(j):
        compute(first, 0, j // 2, j % 2)

    writes = pltpu.make_async_copy(total, out.at[0], out_sem)
    writes.start()

    for j in range(1, n):
        g_send(j).wait_send()

    @pl.loop(0, n)
    def _(j):
        partner(j, r).wait_send()

    ring_sent(m, c)

    @pl.loop(0, m)
    def _(d):
        at_distance(d, ring_sent)

    def z_sent(item, tok):
        @pl.loop(0, m)
        def _(col):
            @pl.when((col <= c) & up)
            def _():
                z_copy(item, tok, col, 0).wait_send()

            @pl.when((col >= c) & down)
            def _():
                z_copy(item, tok, col, 1).wait_send()

    z_sent(0, k)
    for j in range(n):
        z_sent(1 + j, member(j))
    writes.wait()


def body(n, m, activations, grads_t):
    _, units, chunk = grads_t.shape
    rows, wide = activations.shape
    tokens = rows * n * m
    dma = pltpu.SemaphoreType.DMA
    return pl.pallas_call(
        functools.partial(kernel, n, m),
        out_shape=jax.ShapeDtypeStruct((1, units, wide), jnp.float32),
        in_specs=[pl.BlockSpec(memory_space=pl.ANY)] * 2,
        out_specs=pl.BlockSpec(memory_space=pl.ANY),
        scratch_shapes=[
            pltpu.VMEM((2, tokens, wide // 4), jnp.bfloat16),
            pltpu.VMEM((2, tokens, wide // 4), jnp.bfloat16),
            pltpu.VMEM((n, 2, units, chunk), jnp.bfloat16),
            pltpu.VMEM((units, wide), jnp.float32),
            dma((5,)),
            dma((2, n + 1, m)),
            dma((n + 1, m)),
            dma((2, m + 1, n, 2)),
            dma((m + 1, n, 2)),
            dma((n,)),
            dma((n, 2)),
            dma((n,)),
            dma,
        ],
        compiler_params=pltpu.CompilerParams(
            collective_id=0, has_side_effects=True, vmem_limit_bytes=60 * 2**20),
    )(activations, grads_t)


def solution(mesh):
    return jax.shard_map(
        functools.partial(body, mesh.shape["tok"], mesh.shape["col"]),
        mesh=mesh,
        in_specs=(P(("tok", "col"), "row"), P(None, "col", ("tok", "row"))),
        out_specs=P("tok", "col", "row"),
        check_vma=False,
    )
```

```python
import functools

import jax
import jax.numpy as jnp
from jax import lax
from jax.experimental import pallas as pl
from jax.experimental.pallas import tpu as pltpu
from jax.sharding import PartitionSpec as P

MESH = pl.DeviceIdType.MESH


def ring_map(place, n):
    if n % 4:
        return place
    return place + ((place % 4) // 2) * (1 - 2 * (place % 2))


def kernel(n, m, acts, grads, every, held, stage, stage_g,
           local_sem, zsend, zrecv, rsend, rrecv, gsend, grecv, psend):
    k, r, c = lax.axis_index("tok"), lax.axis_index("row"), lax.axis_index("col")
    place = ring_map(k, n)
    rows, wide = acts.shape
    quarter = wide // 4
    chunk = grads.shape[2]
    up, down = c + 1 < m, c > 0
    reach = ((n // 2, n - 1 - n // 2), (n - 1 - n // 2, n // 2))
    hops = n // 2

    def member(offset):
        return ring_map((place + offset + 2 * n) % n, n)

    barrier = pltpu.get_barrier_semaphore()
    for j in range(1, n):
        pl.semaphore_signal(barrier, inc=1, device_id={"tok": (k + j) % n}, device_id_type=MESH)
    pl.semaphore_signal(barrier, inc=1, device_id={"row": 1 - r}, device_id_type=MESH)

    @pl.when(up)
    def _():
        pl.semaphore_signal(barrier, inc=1, device_id={"col": c + 1}, device_id_type=MESH)

    @pl.when(down)
    def _():
        pl.semaphore_signal(barrier, inc=1, device_id={"col": c - 1}, device_id_type=MESH)

    def span(tok, col):
        return pl.ds(pl.multiple_of((tok * m + col) * rows, rows), rows)

    def at_slot(tok, side):
        return held.at[:, pl.ds(pl.multiple_of((tok * 2 + side) * chunk, chunk), chunk)]

    own = every.at[span(k, c), :]
    enter = pltpu.make_async_copy(acts, stage, local_sem.at[0])
    enter_g = pltpu.make_async_copy(grads.at[k], stage_g, local_sem.at[1])
    leave = pltpu.make_async_copy(stage, own, local_sem.at[2])
    leave_g = pltpu.make_async_copy(stage_g, at_slot(k, r), local_sem.at[3])

    @pl.when(up & down)
    def _():
        pl.semaphore_wait(barrier, n + 2)

    @pl.when(jnp.logical_not(up & down))
    def _():
        pl.semaphore_wait(barrier, n + 1)

    def z_copy(item, tok, col, way, fresh=False):
        begin = 0 if isinstance(item, int) and item == 0 else 2 * quarter
        cols = pl.ds(begin, 2 * quarter)
        where = every.at[span(tok, col), cols]
        return pltpu.make_async_remote_copy(
            acts.at[:, cols] if fresh else where, where,
            zsend.at[way, item, col], zrecv.at[item, col],
            device_id={"col": c + 1 - 2 * way}, device_id_type=MESH)

    def z_start(item, tok, fresh=False):
        @pl.when(up)
        def _():
            z_copy(item, tok, c, 0, fresh).start()

        @pl.when(down)
        def _():
            z_copy(item, tok, c, 1, fresh).start()

    def z_round(s, item, tok):
        below, above = c - 1 - s, c + 1 + s

        @pl.when(below >= 0)
        def _():
            z_copy(item, tok, below, 0).wait_recv()

            @pl.when(up)
            def _():
                z_copy(item, tok, below, 0).start()

        @pl.when(above < m)
        def _():
            z_copy(item, tok, above, 1).wait_recv()

            @pl.when(down)
            def _():
                z_copy(item, tok, above, 1).start()

    def ring_copy(line, col, offset, half, way, fresh=False):
        begin = 2 * quarter if isinstance(line, int) and line == m else 0
        cols = pl.ds(begin + half * quarter, quarter)
        tok = member(offset)
        where = every.at[span(tok, col), cols]
        return pltpu.make_async_remote_copy(
            acts.at[:, cols] if fresh else where, where,
            rsend.at[way, line, tok, half], rrecv.at[line, tok, half],
            device_id={"tok": member(1 - 2 * way)}, device_id_type=MESH)

    def ring_start(line, col, fresh=False):
        for half in range(2):
            for way in range(2):
                which = half if way == 0 else 1 - half
                if reach[which][way] >= 1:
                    ring_copy(line, col, 0, which, way, fresh).start()

    def ring_step(line, col, t):
        for half in range(2):
            for way in range(2):
                which = half if way == 0 else 1 - half
                if reach[which][way] >= t:
                    offset = -t if way == 0 else t
                    ring_copy(line, col, offset, which, way).wait_recv()
                    if reach[which][way] > t:
                        ring_copy(line, col, offset, which, way).start()

    def ring_sent(line, col):
        for half in range(2):
            for way in range(2):
                for t in range(reach[half][way]):
                    ring_copy(line, col, -t if way == 0 else t, half, way).wait_send()

    def at_distance(d, do):
        @pl.when(c - d >= 0)
        def _():
            do(c - d, c - d)

        @pl.when((c + d < m) & (d > 0))
        def _():
            do(c + d, c + d)

    def g_send(j):
        to = (k + j) % n
        return pltpu.make_async_remote_copy(
            grads.at[to], at_slot(k, r), gsend.at[j], grecv.at[k, r],
            device_id={"tok": to}, device_id_type=MESH)

    def g_recv(tok):
        where = at_slot(tok, r)
        return pltpu.make_async_remote_copy(
            where, where, gsend.at[0], grecv.at[tok, r],
            device_id={"row": 1 - r}, device_id_type=MESH)

    def partner(tok, side, fresh=False):
        where = at_slot(tok, side)
        return pltpu.make_async_remote_copy(
            grads.at[tok] if fresh else where, where, psend.at[tok], grecv.at[tok, side],
            device_id={"row": 1 - r}, device_id_type=MESH)

    ring_start(m, c, True)
    z_start(0, k, True)
    z_start(1, k, True)
    ring_start(c, c, True)
    partner(k, r, True).start()
    enter.start()
    enter_g.start()
    enter.wait()
    leave.start()
    enter_g.wait()
    leave_g.start()
    for t in range(1, hops + 1):
        ring_step(m, c, t)
        if t == 1:
            for j in sorted(range(1, n), key=lambda j: (min(j, n - j), j)):
                g_send(j).start()
        z_start(1 + (n - t), member(-t))
        if 2 * t != n:
            z_start(1 + t, member(t))

    def item_order():
        order = [0]
        for t in range(1, hops + 1):
            order.append(n - t)
            if 2 * t != n:
                order.append(t)
        return order

    def whole_round(s):
        z_round(s, 0, k)
        at_distance(s + 1, ring_start)
        for j in item_order():
            z_round(s, 1 + j, member(j))

    @pl.loop(0, m - 2)
    def _(s):
        whole_round(s)

    for j in sorted(range(1, n), key=lambda j: (min(j, n - j), j)):
        tok = (k + n - j) % n
        g_recv(tok).wait_recv()
        partner(tok, r).start()

    @pl.loop(0, m - 1)
    def _(d):
        at_distance(d, functools.partial(ring_step, t=1))

    @pl.loop(0, n)
    def _(j):
        partner((k + j) % n, 1 - r).wait_recv()

    z_round(m - 2, 0, k)
    at_distance(m - 1, ring_start)
    at_distance(m - 1, functools.partial(ring_step, t=1))
    for j in item_order():
        z_round(m - 2, 1 + j, member(j))
    for t in range(2, hops + 1):
        @pl.loop(0, m)
        def _(d):
            at_distance(d, functools.partial(ring_step, t=t))

    for j in range(1, n):
        g_send(j).wait_send()

    @pl.loop(0, n)
    def _(j):
        partner(j, r).wait_send()

    ring_sent(m, c)

    @pl.loop(0, m)
    def _(d):
        at_distance(d, ring_sent)

    def z_sent(item, tok):
        @pl.loop(0, m)
        def _(col):
            @pl.when((col <= c) & up)
            def _():
                z_copy(item, tok, col, 0).wait_send()

            @pl.when((col >= c) & down)
            def _():
                z_copy(item, tok, col, 1).wait_send()

    z_sent(0, k)
    for j in range(n):
        z_sent(1 + j, member(j))
    leave.wait()
    leave_g.wait()


def body(n, m, activations, grads_t):
    _, units, chunk = grads_t.shape
    rows, wide = activations.shape
    tokens = rows * n * m
    dma = pltpu.SemaphoreType.DMA
    every, held = pl.pallas_call(
        functools.partial(kernel, n, m),
        out_shape=(
            jax.ShapeDtypeStruct((tokens, wide), jnp.bfloat16),
            jax.ShapeDtypeStruct((units, n * 2 * chunk), jnp.bfloat16),
        ),
        in_specs=[pl.BlockSpec(memory_space=pl.ANY)] * 2,
        out_specs=[pl.BlockSpec(memory_space=pl.ANY)] * 2,
        scratch_shapes=[
            pltpu.VMEM((rows, wide), jnp.bfloat16),
            pltpu.VMEM((units, chunk), jnp.bfloat16),
            dma((4,)),
            dma((2, n + 1, m)),
            dma((n + 1, m)),
            dma((2, m + 1, n, 2)),
            dma((m + 1, n, 2)),
            dma((n,)),
            dma((n, 2)),
            dma((n,)),
        ],
        compiler_params=pltpu.CompilerParams(
            collective_id=0, has_side_effects=True, vmem_limit_bytes=60 * 2**20),
    )(activations, grads_t)
    return jnp.dot(held, every, preferred_element_type=jnp.float32)[None]


def solution(mesh):
    return jax.shard_map(
        functools.partial(body, mesh.shape["tok"], mesh.shape["col"]),
        mesh=mesh,
        in_specs=(P(("tok", "col"), "row"), P(None, "col", ("tok", "row"))),
        out_specs=P("tok", "col", "row"),
        check_vma=False,
    )
```

```python
import functools

import jax
import jax.numpy as jnp
from jax import lax
from jax.experimental import pallas as pl
from jax.experimental.pallas import tpu as pltpu
from jax.sharding import PartitionSpec as P

MESH = pl.DeviceIdType.MESH


def ring_map(place, n):
    if n % 4:
        return place
    return place + ((place % 4) // 2) * (1 - 2 * (place % 2))


def kernel(n, m, acts, grads, every, held, stage, stage_g,
           local_sem, zsend, zrecv, rsend, rrecv, gsend, grecv, psend):
    k, r, c = lax.axis_index("tok"), lax.axis_index("row"), lax.axis_index("col")
    place = ring_map(k, n)
    rows, wide = acts.shape
    quarter = wide // 4
    chunk = grads.shape[2]
    up, down = c + 1 < m, c > 0
    reach = ((n // 2, n - 1 - n // 2), (n - 1 - n // 2, n // 2))
    hops = n // 2

    def member(offset):
        return ring_map((place + offset + 2 * n) % n, n)

    barrier = pltpu.get_barrier_semaphore()
    for j in range(1, n):
        pl.semaphore_signal(barrier, inc=1, device_id={"tok": (k + j) % n}, device_id_type=MESH)
    pl.semaphore_signal(barrier, inc=1, device_id={"row": 1 - r}, device_id_type=MESH)

    @pl.when(up)
    def _():
        pl.semaphore_signal(barrier, inc=1, device_id={"col": c + 1}, device_id_type=MESH)

    @pl.when(down)
    def _():
        pl.semaphore_signal(barrier, inc=1, device_id={"col": c - 1}, device_id_type=MESH)

    def span(tok, col):
        return pl.ds(pl.multiple_of((tok * m + col) * rows, rows), rows)

    def at_slot(tok, side):
        return held.at[:, pl.ds(pl.multiple_of((tok * 2 + side) * chunk, chunk), chunk)]

    own = every.at[span(k, c), :]
    enter = pltpu.make_async_copy(acts, stage, local_sem.at[0])
    enter_g = pltpu.make_async_copy(grads.at[k], stage_g, local_sem.at[1])
    leave = pltpu.make_async_copy(stage, own, local_sem.at[2])
    leave_g = pltpu.make_async_copy(stage_g, at_slot(k, r), local_sem.at[3])

    @pl.when(up & down)
    def _():
        pl.semaphore_wait(barrier, n + 2)

    @pl.when(jnp.logical_not(up & down))
    def _():
        pl.semaphore_wait(barrier, n + 1)

    def z_copy(item, tok, col, way, fresh=False):
        begin = 0 if isinstance(item, int) and item == 0 else 2 * quarter
        cols = pl.ds(begin, 2 * quarter)
        where = every.at[span(tok, col), cols]
        return pltpu.make_async_remote_copy(
            acts.at[:, cols] if fresh else where, where,
            zsend.at[way, item, col], zrecv.at[item, col],
            device_id={"col": c + 1 - 2 * way}, device_id_type=MESH)

    def z_start(item, tok, fresh=False):
        @pl.when(up)
        def _():
            z_copy(item, tok, c, 0, fresh).start()

        @pl.when(down)
        def _():
            z_copy(item, tok, c, 1, fresh).start()

    def z_round(s, item, tok):
        below, above = c - 1 - s, c + 1 + s

        @pl.when(below >= 0)
        def _():
            z_copy(item, tok, below, 0).wait_recv()

            @pl.when(up)
            def _():
                z_copy(item, tok, below, 0).start()

        @pl.when(above < m)
        def _():
            z_copy(item, tok, above, 1).wait_recv()

            @pl.when(down)
            def _():
                z_copy(item, tok, above, 1).start()

    def ring_copy(line, col, offset, half, way, fresh=False):
        begin = 2 * quarter if isinstance(line, int) and line == m else 0
        cols = pl.ds(begin + half * quarter, quarter)
        tok = member(offset)
        where = every.at[span(tok, col), cols]
        return pltpu.make_async_remote_copy(
            acts.at[:, cols] if fresh else where, where,
            rsend.at[way, line, tok, half], rrecv.at[line, tok, half],
            device_id={"tok": member(1 - 2 * way)}, device_id_type=MESH)

    def ring_start(line, col, fresh=False):
        for half in range(2):
            for way in range(2):
                which = half if way == 0 else 1 - half
                if reach[which][way] >= 1:
                    ring_copy(line, col, 0, which, way, fresh).start()

    def ring_step(line, col, t):
        for half in range(2):
            for way in range(2):
                which = half if way == 0 else 1 - half
                if reach[which][way] >= t:
                    offset = -t if way == 0 else t
                    ring_copy(line, col, offset, which, way).wait_recv()
                    if reach[which][way] > t:
                        ring_copy(line, col, offset, which, way).start()

    def ring_sent(line, col):
        for half in range(2):
            for way in range(2):
                for t in range(reach[half][way]):
                    ring_copy(line, col, -t if way == 0 else t, half, way).wait_send()

    def at_distance(d, do):
        @pl.when(c - d >= 0)
        def _():
            do(c - d, c - d)

        @pl.when((c + d < m) & (d > 0))
        def _():
            do(c + d, c + d)

    def g_send(j):
        to = (k + j) % n
        return pltpu.make_async_remote_copy(
            grads.at[to], at_slot(k, r), gsend.at[j], grecv.at[k, r],
            device_id={"tok": to}, device_id_type=MESH)

    def g_recv(tok):
        where = at_slot(tok, r)
        return pltpu.make_async_remote_copy(
            where, where, gsend.at[0], grecv.at[tok, r],
            device_id={"row": 1 - r}, device_id_type=MESH)

    def partner(tok, side, fresh=False):
        where = at_slot(tok, side)
        return pltpu.make_async_remote_copy(
            grads.at[tok] if fresh else where, where, psend.at[tok], grecv.at[tok, side],
            device_id={"row": 1 - r}, device_id_type=MESH)

    ring_start(m, c, True)
    z_start(0, k, True)
    z_start(1, k, True)
    ring_start(c, c, True)
    partner(k, r, True).start()
    enter.start()
    enter_g.start()
    enter.wait()
    leave.start()
    enter_g.wait()
    leave_g.start()
    for t in range(1, hops + 1):
        ring_step(m, c, t)
        if t == 1:
            for j in sorted(range(1, n), key=lambda j: (min(j, n - j), j)):
                g_send(j).start()
        z_start(1 + (n - t), member(-t))
        if 2 * t != n:
            z_start(1 + t, member(t))

    def item_order():
        order = [0]
        for t in range(1, hops + 1):
            order.append(n - t)
            if 2 * t != n:
                order.append(t)
        return order

    def whole_round(s):
        z_round(s, 0, k)
        at_distance(s + 1, ring_start)
        for j in item_order():
            z_round(s, 1 + j, member(j))

    @pl.loop(0, m - 2)
    def _(s):
        whole_round(s)

    for j in sorted(range(1, n), key=lambda j: (min(j, n - j), j)):
        tok = (k + n - j) % n
        g_recv(tok).wait_recv()
        partner(tok, r).start()

    @pl.loop(0, m - 2)
    def _(d):
        at_distance(d, functools.partial(ring_step, t=1))

    @pl.loop(0, n)
    def _(j):
        partner((k + j) % n, 1 - r).wait_recv()

    z_round(m - 2, 0, k)
    at_distance(m - 1, ring_start)
    at_distance(m - 2, functools.partial(ring_step, t=1))
    at_distance(m - 1, functools.partial(ring_step, t=1))
    for j in item_order():
        z_round(m - 2, 1 + j, member(j))
    for t in range(2, hops + 1):
        @pl.loop(0, m)
        def _(d):
            at_distance(d, functools.partial(ring_step, t=t))

    for j in range(1, n):
        g_send(j).wait_send()

    @pl.loop(0, n)
    def _(j):
        partner(j, r).wait_send()

    ring_sent(m, c)

    @pl.loop(0, m)
    def _(d):
        at_distance(d, ring_sent)

    def z_sent(item, tok):
        @pl.loop(0, m)
        def _(col):
            @pl.when((col <= c) & up)
            def _():
                z_copy(item, tok, col, 0).wait_send()

            @pl.when((col >= c) & down)
            def _():
                z_copy(item, tok, col, 1).wait_send()

    z_sent(0, k)
    for j in range(n):
        z_sent(1 + j, member(j))
    leave.wait()
    leave_g.wait()


def body(n, m, activations, grads_t):
    _, units, chunk = grads_t.shape
    rows, wide = activations.shape
    tokens = rows * n * m
    dma = pltpu.SemaphoreType.DMA
    every, held = pl.pallas_call(
        functools.partial(kernel, n, m),
        out_shape=(
            jax.ShapeDtypeStruct((tokens, wide), jnp.bfloat16),
            jax.ShapeDtypeStruct((units, n * 2 * chunk), jnp.bfloat16),
        ),
        in_specs=[pl.BlockSpec(memory_space=pl.ANY)] * 2,
        out_specs=[pl.BlockSpec(memory_space=pl.ANY)] * 2,
        scratch_shapes=[
            pltpu.VMEM((rows, wide), jnp.bfloat16),
            pltpu.VMEM((units, chunk), jnp.bfloat16),
            dma((4,)),
            dma((2, n + 1, m)),
            dma((n + 1, m)),
            dma((2, m + 1, n, 2)),
            dma((m + 1, n, 2)),
            dma((n,)),
            dma((n, 2)),
            dma((n,)),
        ],
        compiler_params=pltpu.CompilerParams(
            collective_id=0, has_side_effects=True, vmem_limit_bytes=60 * 2**20),
    )(activations, grads_t)
    return jnp.dot(held, every, preferred_element_type=jnp.float32)[None]


def solution(mesh):
    return jax.shard_map(
        functools.partial(body, mesh.shape["tok"], mesh.shape["col"]),
        mesh=mesh,
        in_specs=(P(("tok", "col"), "row"), P(None, "col", ("tok", "row"))),
        out_specs=P("tok", "col", "row"),
        check_vma=False,
    )
```
